32 devices in a mesh: dp: 4 (over y, x), seq: 8 (over z, core).
Axes of the slice: x: 2, y: 2, z: 4, core: 2. Of those that a mesh axis runs over, the one named last changes fastest.
Arguments:
- inputs: bfloat16 [4, 8192, 512], P('dp', 'seq'), may hold values from -0.0014648438 to 0.0014648438
- grad_out: bfloat16 [4, 8192, 512], P('dp', 'seq'), may hold values from -6 to 6
- conv_filter: bfloat16 [8192], P('seq'), may hold values from -0.0625 to 0.0625
Outputs:
- grad_input: bfloat16 [4, 8192, 512], P('dp', 'seq')
- grad_filter: float32 [8192], P('seq')
The draws below stay inside these ranges and needn't reach their ends.
All inputs are finite; a program needn't handle non-finite values.
Results may differ from the reference program's by a relative error of at most 0.0095.
Values may be sent and summed in bfloat16 or wider, within the bound.
No kernel may reach another device: no remote copies, remote signals or barrier semaphores. Data moves between devices by JAX's collectives and lax.ppermute only.
A program may use at most 128 MiB of HBM per device.

```python
import jax
import jax.numpy as jnp
from jax import lax

CH = 512
LEN = 8192
BATCH = 4


def levels(key, extent, pieces, least, top_value):
    loudness, own = 1.0, jax.random.fold_in(key, 6)
    for dim, blocks in pieces:
        steps = jnp.exp(jax.random.uniform(jax.random.fold_in(own, dim), (blocks,), jnp.float32, least / len(pieces), top_value / len(pieces)))
        loudness = loudness * jnp.repeat(steps, extent[dim] // blocks).reshape([-1 if axis == dim else 1 for axis in range(len(extent))])
    return loudness


def noise(key, dims, scale, bound, shards=(), held_as=jnp.bfloat16):
    level = levels(key, dims, shards, -0.22, 0.18) if shards else 1.0
    result = jax.random.normal(key, dims, jnp.float32) * scale * level
    return jnp.minimum(jnp.maximum(result, -bound), bound).astype(held_as)


def setup_inputs(seed: int = 0) -> dict:
    arg_keys = jax.random.split(jax.random.key(seed), 4)
    return {
        "inputs": noise(arg_keys[0], (BATCH, LEN, CH), (LEN * CH * BATCH) ** -0.5, 0.0014648438, ((0, 4), (1, 8))),
        "grad_out": noise(arg_keys[1], (BATCH, LEN, CH), 1.0, 6.0, ((0, 4), (1, 8))),
        "conv_filter": noise(arg_keys[2], (LEN,), LEN ** -0.5, 0.0625, ((0, 8),)),
    }


def reference(inputs, grad_out, conv_filter):
    period = 2 * LEN
    filter_spec = jnp.fft.rfft(conv_filter.astype(jnp.float32), n=period)

    def per_sequence(members):
        seq_inputs, seq_grads = members
        input_spec = jnp.fft.rfft(seq_inputs.astype(jnp.float32), n=period, axis=0)
        grad_spec = jnp.fft.rfft(seq_grads.astype(jnp.float32), n=period, axis=0)
        product = jnp.conj(filter_spec)[:, None] * grad_spec
        backward = jnp.fft.irfft(product, n=period, axis=0)[:LEN]
        filter_term = jnp.sum(grad_spec * jnp.conj(input_spec), axis=1)
        return backward.astype(jnp.bfloat16), filter_term

    grad_input, filter_terms = lax.map(per_sequence, (inputs, grad_out))
    grad_filter = jnp.fft.irfft(jnp.sum(filter_terms, axis=0), n=period)[:LEN].astype(jnp.float32)
    return grad_input, grad_filter
```

```python
import jax
import jax.numpy as jnp
from jax import lax
from jax.experimental import pallas as pl
from jax.experimental.pallas import tpu as pltpu
from jax.sharding import PartitionSpec as P

TILE = 256


def low_bit(value):
    return value & -value


def reach(chip, core, chips):
    span = low_bit(chip + 1) if core == 0 else low_bit(chip)
    return span if span < chips else 0


def place(chips):
    index = lax.axis_index("seq")
    chip, core = index // 2, index % 2
    span = jnp.where(core == 0, low_bit(chip + 1), low_bit(chip))
    return core, jnp.where(span < chips, span, 0)


def hops(chips, distance, kind):
    pairs = []
    for chip in range(chips):
        for core in range(2):
            span = reach(chip, core, chips)
            own_first = span - 1
            limit = {"grad": (span, own_first), "rest": (own_first, span)}[kind][core]
            if distance <= limit:
                pairs.append((chip, core))
    return pairs


def levels_of(most):
    level = 1
    while level <= most:
        yield level
        level *= 2


def dot(left, right):
    return jnp.dot(left, right, preferred_element_type=jnp.float32)


def dot_nt(left, right):
    return lax.dot_general(left, right, (((1,), (1,)), ((), ())), preferred_element_type=jnp.float32)


def local_kernel(filter_ref, grad_ref, input_ref, stair_ref, out_ref, lag_ref, skew_ref):
    slab = grad_ref.shape[0]
    length = stair_ref.shape[1]
    width = skew_ref.shape[1]
    row = jnp.broadcast_to(filter_ref[...], (8, width))
    skew_ref[...] = pltpu.roll(row, 0, 1, stride=1, stride_axis=0)

    def rows(step, carry):
        low = skew_ref[...]
        high = pltpu.roll(low, 8, 1)
        both = jnp.concatenate([low[:, :length], high[:, :length]], axis=0)
        stair_ref[pl.ds(pl.multiple_of(step * 16, 16), 16), :] = both.astype(stair_ref.dtype)
        skew_ref[...] = pltpu.roll(high, 8, 1)
        return carry

    lax.fori_loop(0, TILE // 16, rows, 0)
    lag_ref[...] = jnp.zeros_like(lag_ref)
    for start in range(0, slab, TILE):
        rest = grad_ref[start:, :]
        out_ref[start : start + TILE, :] = dot(stair_ref[:, : slab - start], rest)
        lag_ref[:, : slab - start] += dot_nt(input_ref[start : start + TILE, :], rest)


def sources(core, own, received):
    return list(received) if core == 0 else [own, *received[:-1]]


def cross_kernel(chips, stair_ref, grad_ref, *refs):
    most = chips // 2
    received, sent, kept_ref = refs[:most], refs[most : 2 * most], refs[2 * most]
    slab = grad_ref.shape[0]
    blocks = slab // TILE
    core, span = place(chips)

    @pl.when((core == 1) | (span == 0))
    def _():
        kept_ref[...] = jnp.zeros_like(kept_ref)

    for side in range(2):
        grads = sources(side, grad_ref, received)
        targets = [kept_ref, *sent[:-1]] if side == 0 else list(sent)
        for level in levels_of(most):

            @pl.when((core == side) & (span == level))
            def _(grads=grads, targets=targets, level=level):
                for low in range(level):

                    def block(step, carry, low=low):
                        lag = low * blocks + blocks - step
                        total = 0.0
                        for high in range(level):
                            at = pl.multiple_of((lag + high * blocks) * TILE, TILE)
                            total += dot(stair_ref[:, pl.ds(at, slab)], grads[high][...])
                        rows = pl.ds(pl.multiple_of(step * TILE, TILE), TILE)
                        targets[low][rows, :] = total.astype(targets[low].dtype)
                        return carry

                    lax.fori_loop(0, blocks, block, 0)


def lag_kernel(chips, local_ref, grad_ref, input_ref, *refs):
    most = chips // 2
    got_grads, got_inputs = refs[:most], refs[most : 2 * most]
    out_ref, lag_ref, skew_ref = refs[2 * most :]
    slab = grad_ref.shape[0]
    blocks = slab // TILE
    length = lag_ref.shape[1]
    core, span = place(chips)
    lag_ref[:, :slab] = local_ref[...]
    lag_ref[:, slab:] = jnp.zeros((TILE, length - slab), jnp.float32)
    for side in range(2):
        grads = sources(side, grad_ref, got_grads)
        inputs = sources(1 - side, input_ref, got_inputs)
        for level in levels_of(most):

            @pl.when((core == side) & (span == level))
            def _(grads=grads, inputs=inputs, level=level):
                for low in range(level):

                    def block(step, carry, low=low):
                        lag = low * blocks + blocks - step
                        rows = pl.ds(pl.multiple_of(step * TILE, TILE), TILE)
                        left = inputs[low][rows, :]
                        for high in range(level):
                            at = pl.multiple_of((lag + high * blocks) * TILE, TILE)
                            lag_ref[:, pl.ds(at, slab)] += dot_nt(left, grads[high][...])
                        return carry

                    lax.fori_loop(0, blocks, block, 0)

    width = skew_ref.shape[1]
    skew_ref[...] = jnp.zeros_like(skew_ref)

    def rows(step, carry):
        group = TILE // 8 - 1 - step
        moved = pltpu.roll(skew_ref[...], width - 8, 1)
        part = lag_ref[pl.ds(pl.multiple_of(group * 8, 8), 8), :]
        skew_ref[...] = moved + jnp.concatenate([part, jnp.zeros((8, width - length), jnp.float32)], axis=1)
        return carry

    lax.fori_loop(0, TILE // 8, rows, 0)
    total = skew_ref[0:1, :]
    for row in range(1, 8):
        total += pltpu.roll(skew_ref[row : row + 1, :], width - row, 1)
    out_ref[...] = total[:, :length]


def finish_kernel(local_ref, kept_ref, *refs):
    total = local_ref[...] + kept_ref[...].astype(jnp.float32)
    for ref in refs[:-1]:
        total += ref[...].astype(jnp.float32)
    refs[-1][...] = total.astype(refs[-1].dtype)


def call(kernel, outs, scratch=()):
    return pl.pallas_call(kernel, out_shape=outs, scratch_shapes=scratch)


def on_device(inputs, grad_out, conv_filter):
    shards = lax.axis_size("seq")
    chips = shards // 2
    most = chips // 2
    core = lax.axis_index("seq") % 2
    tokens, channels = inputs.shape[1], inputs.shape[2]
    half = channels // 2
    slab = 2 * tokens
    length = shards * tokens
    swap = [(index, index ^ 1) for index in range(shards)]

    def to_slab(array):
        mine = lax.dynamic_slice_in_dim(array[0], core * half, half, 1)
        other = lax.dynamic_slice_in_dim(array[0], (1 - core) * half, half, 1)
        other = lax.ppermute(other, "seq", swap)
        return jnp.where(
            core == 0, jnp.concatenate([mine, other], 0), jnp.concatenate([other, mine], 0)
        )

    def shift(array, distance, kind, sign):
        pairs = []
        for chip, side in hops(chips, distance, kind):
            away = 2 * (chip + distance * (1 if kind == "grad" else -1)) + side
            here = 2 * chip + side
            pairs.append((away, here) if sign > 0 else (here, away))
        return lax.ppermute(array, "seq", pairs) if pairs else jnp.zeros_like(array)

    whole_filter = lax.all_gather(conv_filter, "seq", tiled=True)
    grads = to_slab(grad_out)
    values = to_slab(inputs)
    got_grads = [shift(grads, distance, "grad", 1) for distance in range(1, most + 1)]
    got_values = [shift(values, distance, "rest", 1) for distance in range(1, most + 1)]
    row = jnp.pad(whole_filter.astype(jnp.float32).reshape(1, length), ((0, 0), (0, TILE)))
    stair, local_out, local_lag = call(
        local_kernel,
        (
            jax.ShapeDtypeStruct((TILE, length), jnp.bfloat16),
            jax.ShapeDtypeStruct((slab, half), jnp.float32),
            jax.ShapeDtypeStruct((TILE, slab), jnp.float32),
        ),
        (pltpu.VMEM((8, length + TILE), jnp.float32),),
    )(row, grads, values)
    piece = jax.ShapeDtypeStruct((slab, half), jnp.bfloat16)
    *sent, kept = call(
        lambda *refs: cross_kernel(chips, *refs),
        (*([piece] * most), jax.ShapeDtypeStruct((slab, half), jnp.float32)),
    )(stair, grads, *got_grads)
    parts = [shift(array, index + 1, "rest", -1) for index, array in enumerate(sent)]
    filter_part = call(
        lambda *refs: lag_kernel(chips, *refs),
        jax.ShapeDtypeStruct((1, length), jnp.float32),
        (pltpu.VMEM((TILE, length), jnp.float32), pltpu.VMEM((8, length + TILE), jnp.float32)),
    )(local_lag, grads, values, *got_grads, *got_values)
    spread = lax.all_to_all(filter_part.reshape(shards, tokens), "seq", 0, 0, tiled=True)
    grad_filter = jnp.sum(lax.all_gather(jnp.sum(spread, axis=0), "dp"), axis=0)
    result = call(finish_kernel, piece)(local_out, kept, *parts)
    mine = lax.dynamic_slice_in_dim(result, core * tokens, tokens, 0)
    other = lax.dynamic_slice_in_dim(result, (1 - core) * tokens, tokens, 0)
    other = lax.ppermute(other, "seq", swap)
    grad_input = jnp.where(
        core == 0, jnp.concatenate([mine, other], 1), jnp.concatenate([other, mine], 1)
    )
    return grad_input[None], grad_filter


def solution(mesh):
    placed = (P("dp", "seq", None), P("dp", "seq", None), P("seq"))
    return jax.shard_map(
        on_device,
        mesh=mesh,
        in_specs=placed,
        out_specs=(P("dp", "seq", None), P("seq")),
        check_vma=False,
    )
```

```python
import jax
import jax.numpy as jnp
from jax import lax
from jax.experimental import pallas as pl
from jax.experimental.pallas import tpu as pltpu
from jax.sharding import PartitionSpec as P


TILE = 256


def low_bit(value):
    return value & -value


def reach(chip, core, chips):
    span = low_bit(chip + 1) if core == 0 else low_bit(chip)
    return span if span < chips else 0


def place(chips):
    index = lax.axis_index("seq")
    chip, core = index // 2, index % 2
    span = jnp.where(core == 0, low_bit(chip + 1), low_bit(chip))
    return core, jnp.where(span < chips, span, 0)


def levels_of(most):
    level = 1
    while level <= most:
        yield level
        level *= 2


def dot(left, right):
    return jnp.dot(left, right, preferred_element_type=jnp.float32)


def dot_nt(left, right):
    return lax.dot_general(left, right, (((1,), (1,)), ((), ())), preferred_element_type=jnp.float32)


def ordered(side, mine, other):
    return [mine, other] if side == 0 else [other, mine]


def paired(side, refs):
    return [ordered(side, refs[at], refs[at + 1]) for at in range(0, len(refs), 2)]


def wide(stair_ref, at, pieces):
    tokens = pieces[0].shape[0]
    total = 0.0
    for index, piece in enumerate(pieces):
        total += dot(stair_ref[:, pl.ds(at + index * tokens, tokens)], piece[...])
    return total


def row_block(pieces, block):
    tokens = pieces[0].shape[0]
    start = block * TILE
    return pieces[start // tokens], start % tokens


def local_kernel(chips, filter_ref, *refs):
    grad_refs, input_refs = refs[0:2], refs[2:4]
    stair_ref, out_ref, lag_ref, early_same_ref, early_other_ref, skew_ref = refs[4:]
    tokens = grad_refs[0].shape[0]
    slab = 2 * tokens
    blocks = slab // TILE
    length = stair_ref.shape[1]
    width = skew_ref.shape[1]
    core, span = place(chips)
    row = jnp.broadcast_to(filter_ref[...], (8, width))
    skew_ref[...] = pltpu.roll(row, 0, 1, stride=1, stride_axis=0)

    def rows(step, carry):
        low = skew_ref[...]
        high = pltpu.roll(low, 8, 1)
        both = jnp.concatenate([low[:, :length], high[:, :length]], axis=0)
        stair_ref[pl.ds(pl.multiple_of(step * 16, 16), 16), :] = both.astype(stair_ref.dtype)
        skew_ref[...] = pltpu.roll(high, 8, 1)
        return carry

    lax.fori_loop(0, TILE // 16, rows, 0)
    lag_ref[...] = jnp.zeros_like(lag_ref)
    for side in range(2):

        @pl.when(core == side)
        def _(side=side):
            grads = ordered(side, *grad_refs)
            values = ordered(side, *input_refs)
            for block in range(blocks):
                start = block * TILE
                value_ref, row = row_block(values, block)
                left = value_ref[row : row + TILE, :]
                total = 0.0
                for index, piece in enumerate(grads):
                    skip = max(start - index * tokens, 0)
                    if skip >= tokens:
                        continue
                    at = index * tokens + skip - start
                    span_len = tokens - skip
                    right = piece[skip:, :]
                    total += dot(stair_ref[:, at : at + span_len], right)
                    lag_ref[:, at : at + span_len] += dot_nt(left, right)
                out_ref[start : start + TILE, :] = total

    @pl.when((core == 1) & (span == 1))
    def _():
        grads = ordered(1, *grad_refs)
        targets = ordered(1, early_same_ref, early_other_ref)
        for block in range(blocks):
            target, row = row_block(targets, block)
            part = wide(stair_ref, (blocks - block) * TILE, grads)
            target[row : row + TILE, :] = part.astype(target.dtype)


def grads_of(side, own, received):
    return received if side == 0 else [own, *received[:-1]]


def inputs_of(side, own, received):
    return [own, *received[:-1]] if side == 0 else received


def partial_rows(stair_ref, grads, low, blocks, step):
    lag = low * blocks + blocks - step
    total = 0.0
    for high, pieces in enumerate(grads):
        at = pl.multiple_of((lag + high * blocks) * TILE, TILE)
        total += wide(stair_ref, at, pieces)
    return total


def cross_kernel(chips, first, stair_ref, *refs):
    most = chips // 2
    own, received = refs[0:2], refs[2 : 2 + 2 * most]
    tokens = own[0].shape[0]
    blocks = 2 * tokens // TILE
    per = tokens // TILE
    core, span = place(chips)
    if first:
        sent = refs[2 + 2 * most :]
    else:
        local_ref = refs[2 + 2 * most]
        keep_ref, give_ref = refs[3 + 2 * most : 5 + 2 * most]
        sent = refs[5 + 2 * most :]

    for side in range(2):
        grads = grads_of(side, ordered(side, *own), paired(side, received))
        targets = paired(side, sent)
        mine = [keep_ref, give_ref] if not first else None

        def put(pieces, low, level, local=False, grads=grads, side=side):
            for index, piece in enumerate(pieces):

                def block(step, carry, index=index, piece=piece):
                    step = step + index * per
                    if level:
                        total = partial_rows(stair_ref, grads[:level], low, blocks, step)
                    else:
                        total = 0.0
                    if local:
                        total += local_ref[pl.ds(pl.multiple_of(step * TILE, TILE), TILE), :]
                    rows = pl.ds(pl.multiple_of((step - index * per) * TILE, TILE), TILE)
                    piece[rows, :] = total.astype(piece.dtype)
                    return carry

                lax.fori_loop(0, per, block, 0)

        for level in levels_of(most):

            @pl.when((core == side) & (span == level))
            def _(level=level, put=put, targets=targets, mine=mine, side=side):
                if level > 1:
                    if first:
                        put(targets[0], 1 if side == 0 else 0, level)
                    else:
                        for index, pieces in enumerate(targets):
                            low = index + (2 if side == 0 else 1)
                            if low < level:
                                put(pieces, low, level)
                if not first and side == 0:
                    put(ordered(side, *mine), 0, level, True)

        if not first:

            @pl.when((core == side) & ((side == 1) | (span == 0)))
            def _(put=put, mine=mine, side=side):
                put(ordered(side, *mine), 0, 0, True)


def lag_kernel(chips, local_ref, *refs):
    most = chips // 2
    own_grads, own_inputs = refs[0:2], refs[2:4]
    got_grads, got_inputs = refs[4 : 4 + 2 * most], refs[4 + 2 * most : 4 + 4 * most]
    out_ref, lag_ref, skew_ref = refs[4 + 4 * most :]
    tokens = own_grads[0].shape[0]
    slab = 2 * tokens
    blocks = slab // TILE
    per = tokens // TILE
    length = lag_ref.shape[1]
    core, span = place(chips)
    lag_ref[:, :slab] = local_ref[...]
    lag_ref[:, slab:] = jnp.zeros((TILE, length - slab), jnp.float32)
    for side in range(2):
        grads = grads_of(side, ordered(side, *own_grads), paired(side, got_grads))
        values = inputs_of(side, ordered(side, *own_inputs), paired(side, got_inputs))
        for level in levels_of(most):

            @pl.when((core == side) & (span == level))
            def _(grads=grads, values=values, level=level):
                for low in range(level):
                    for index, piece in enumerate(values[low]):

                        def block(step, carry, low=low, index=index, piece=piece):
                            rows = pl.ds(pl.multiple_of(step * TILE, TILE), TILE)
                            left = piece[rows, :]
                            lag = low * blocks + blocks - step - index * per
                            for high in range(level):
                                for part, right in enumerate(grads[high]):
                                    at = (lag + high * blocks + part * per) * TILE
                                    at = pl.multiple_of(at, TILE)
                                    lag_ref[:, pl.ds(at, tokens)] += dot_nt(left, right[...])
                            return carry

                        lax.fori_loop(0, per, block, 0)

    width = skew_ref.shape[1]
    skew_ref[...] = jnp.zeros_like(skew_ref)

    def rows(step, carry):
        group = TILE // 8 - 1 - step
        moved = pltpu.roll(skew_ref[...], width - 8, 1)
        part = lag_ref[pl.ds(pl.multiple_of(group * 8, 8), 8), :]
        skew_ref[...] = moved + jnp.concatenate([part, jnp.zeros((8, width - length), jnp.float32)], axis=1)
        return carry

    lax.fori_loop(0, TILE // 8, rows, 0)
    total = skew_ref[0:1, :]
    for row in range(1, 8):
        total += pltpu.roll(skew_ref[row : row + 1, :], width - row, 1)
    out_ref[...] = total[:, :length]


def finish_kernel(chips, keep_ref, given_ref, *refs):
    core, _ = place(chips)
    out_ref = refs[-1]
    half = keep_ref.shape[1]

    def total(first, parts):
        result = first[...].astype(jnp.float32)
        for part in parts:
            result += part[...].astype(jnp.float32)
        return result.astype(out_ref.dtype)

    for side in range(2):

        @pl.when(core == side)
        def _(side=side):
            mine, other = side * half, (1 - side) * half
            out_ref[:, mine : mine + half] = total(keep_ref, refs[0:-1:2])
            out_ref[:, other : other + half] = total(given_ref, refs[1:-1:2])


def call(kernel, outs, flops, scratch=()):
    return pl.pallas_call(
        kernel,
        out_shape=outs,
        scratch_shapes=scratch,
        cost_estimate=pl.CostEstimate(flops=flops, transcendentals=0, bytes_accessed=0),
    )


def on_device(inputs, grad_out, conv_filter):
    shards = lax.axis_size("seq")
    chips = shards // 2
    most = chips // 2
    core = lax.axis_index("seq") % 2
    tokens, channels = inputs.shape[1], inputs.shape[2]
    half = channels // 2
    slab = 2 * tokens
    length = shards * tokens

    def halves(array):
        return [
            lax.dynamic_slice_in_dim(array[0], start * half, half, 1) for start in (core, 1 - core)
        ]

    def swap(array):
        return lax.ppermute(array, "seq", [(index, index ^ 1) for index in range(shards)])

    def shift(pieces, distance, limit, down):
        results = []
        for turn, piece in enumerate(pieces):
            pairs = []
            for chip in range(chips):
                for side in range(2):
                    if distance > limit(reach(chip, side, chips), side):
                        continue
                    pivot = 2 * chip + side
                    if down == "out":
                        pairs.append((pivot, 2 * (chip - distance) + (side ^ turn)))
                    else:
                        away = chip + distance if down == "grad" else chip - distance
                        pairs.append((2 * away + (side ^ turn), pivot))
            results.append(lax.ppermute(piece, "seq", pairs) if pairs else jnp.zeros_like(piece))
        return results

    grad_limit = lambda span, side: span - side
    rest_limit = lambda span, side: span - 1 + side
    deep_limit = lambda span, side: rest_limit(span, side) if span > 1 else 0
    early_limit = lambda span, side: 1 if span == 1 and side == 1 else 0

    grad_mine, grad_give = halves(grad_out)
    got_grads = {}
    for distance in range(most, 0, -1):
        got_grads[distance] = shift((grad_mine, grad_give), distance, grad_limit, "grad")
    got_grads = [piece for distance in range(1, most + 1) for piece in got_grads[distance]]
    copies = jnp.broadcast_to(conv_filter[None, None], (shards, 1, tokens))
    whole_filter = lax.all_to_all(copies, "seq", 0, 1, tiled=True)
    grads = [grad_mine, swap(grad_give)]
    value_mine, value_give = halves(inputs)
    values = [value_mine, swap(value_give)]
    got_values = []
    for distance in range(1, most + 1):
        got_values += shift((value_mine, value_give), distance, rest_limit, "value")
    row = jnp.pad(whole_filter.astype(jnp.float32).reshape(1, length), ((0, 0), (0, TILE)))
    piece = jax.ShapeDtypeStruct((tokens, half), jnp.bfloat16)
    work = 2 * slab * slab * half
    stair, local_out, local_lag, early_same, early_other = call(
        lambda *refs: local_kernel(chips, *refs),
        (
            jax.ShapeDtypeStruct((TILE, length), jnp.bfloat16),
            jax.ShapeDtypeStruct((slab, half), jnp.float32),
            jax.ShapeDtypeStruct((TILE, slab), jnp.float32),
            piece,
            piece,
        ),
        2 * work,
        (pltpu.VMEM((8, length + TILE), jnp.float32),),
    )(row, *grads, *values)
    parts = shift((early_same, early_other), 1, early_limit, "out")
    sent = call(lambda *refs: cross_kernel(chips, True, *refs), (piece, piece), most * work)(stair, *grads, *got_grads)
    parts += shift(sent, 1, deep_limit, "out")
    keep, give, *sent = call(
        lambda *refs: cross_kernel(chips, False, *refs),
        (jax.ShapeDtypeStruct((tokens, half), jnp.float32), piece, *([piece] * (2 * most - 2))),
        most * work,
    )(stair, *grads, *got_grads, local_out)
    for distance in range(2, most + 1):
        parts += shift(sent[2 * distance - 4 : 2 * distance - 2], distance, deep_limit, "out")
    given = swap(give)
    filter_part = call(
        lambda *refs: lag_kernel(chips, *refs),
        jax.ShapeDtypeStruct((1, length), jnp.float32),
        most * most * work,
        (pltpu.VMEM((TILE, length), jnp.float32), pltpu.VMEM((8, length + TILE), jnp.float32)),
    )(local_lag, *grads, *values, *got_grads, *got_values)
    copies = jnp.broadcast_to(
        filter_part.reshape(1, shards, 1, tokens), (lax.axis_size("dp"), shards, 1, tokens)
    ).reshape(-1, 1, tokens)
    spread = lax.all_to_all(copies, ("dp", "seq"), 0, 1, tiled=True)
    grad_filter = jnp.sum(spread[0], axis=0)
    grad_input = call(
        lambda *refs: finish_kernel(chips, *refs),
        jax.ShapeDtypeStruct((tokens, channels), jnp.bfloat16),
        slab * channels,
    )(keep, given, *parts)
    return grad_input[None], grad_filter


def solution(mesh):
    placed = (P("dp", "seq", None), P("dp", "seq", None), P("seq"))

    return jax.shard_map(
        on_device,
        mesh=mesh,
        in_specs=placed,
        out_specs=(P("dp", "seq", None), P("seq")),
        check_vma=False,
    )
```
